32 devices in a mesh: patch: 32 (over z, y, x, core).
Axes of the slice: x: 2, y: 2, z: 4, core: 2. Of those that a mesh axis runs over, the one named last changes fastest.
Arguments:
- atm_flux: bfloat16 [8, 98304], P(None, 'patch'), may hold values from -6 to 6
- remap_send: int32 [32, 5, 8], P('patch'), may hold values from 0 to 23
- remap_target: int32 [32, 5, 8], P('patch'), may hold values from 0 to 31
- remap_counts: int32 [32, 5], P('patch'), may hold values from 0 to 8, as said below
- remap_weights: bfloat16 [32, 5, 8, 128, 128], P('patch'), may hold values from -0.5 to 0.5
- coupling: float32 [2, 8], replicated, may hold values from -2 to 2
- tracer: float32 [2, 128, 131072], P(None, None, 'patch'), may hold values from -6 to 6
- wet: int32 [131072], P('patch'), may hold values from 0 to 1
- mix_inverse: float32 [1024, 128, 128], P('patch')
- halo_send: int32 [32, 4, 2, 128], P('patch'), may hold values from 0 to 4095
- halo_ghost: int32 [32, 4, 2, 128], P('patch'), may hold values from 0 to 4095
- halo_rows: int32 [32, 4], P('patch'), may hold values from 0 to 2, as said below
Outputs:
- ocean_flux: float32 [8, 131072], P(None, 'patch')
- tracer_out: float32 [2, 128, 131072], P(None, None, 'patch')
The draws below stay inside these ranges and needn't reach their ends.
Inputs may be any that keep to these rules, and one draw needn't show every extreme that they name: `remap_counts`: some entry equals 8. `halo_rows`: some entry equals 2.
All inputs are finite; a program needn't handle non-finite values.
Results may differ from the reference program's by a relative error of at most 0.0003.
Values may be sent and summed in bfloat16 or wider, within the bound.
A program may use at most 64 MiB of HBM per device.

```python
import math
import jax
import jax.numpy as jnp
from jax import lax

F = 8
LEV = 128
NTR = 2
BLOCK = 128
ABLK = 24
OBLK = 32
CAP = 8
REACH = 2
HR = 2
SPAN = 5
HSPAN = 4
OC = 4096
NOC = 131072
NA = 98304
N_PATCH = 32


def force_top(key, rows, columns, top):
    counts = jax.random.randint(jax.random.fold_in(key, 21), (rows * columns,), 0, top + 1)
    spot = jax.random.randint(jax.random.fold_in(key, 22), (), 0, rows * columns)
    counts = jnp.where(jnp.arange(rows * columns) == spot, top, counts)
    return counts.reshape(rows, columns).astype(jnp.int32)


def draw_remap_counts(key, part):
    return force_top(jax.random.fold_in(key, 31), N_PATCH, SPAN, CAP)


def draw_halo_rows(key, part):
    return force_top(jax.random.fold_in(key, 41), N_PATCH, HSPAN, HR)


def draw_wet(key, part):
    percent = jax.random.randint(jax.random.fold_in(key, 51), (N_PATCH, 1), 30, 96)
    rolled = jax.random.randint(jax.random.fold_in(key, 52), (N_PATCH, OBLK * BLOCK), 0, 100)
    return (rolled < percent).astype(jnp.int32).reshape(-1)


def draw_mix_inverse(key, part):
    count = N_PATCH * OBLK
    diag = jax.random.uniform(jax.random.fold_in(key, 61), (count, LEV, 1), jnp.float32, 0.6, 1.4)
    eye = jnp.eye(LEV, dtype=jnp.float32)[None, :, :]
    spread = 0.5 * jax.random.normal(jax.random.fold_in(key, 63), (count, LEV, LEV), jnp.float32)
    return (eye * diag + spread / math.sqrt(LEV)).astype(jnp.float32)


def plant(values, stream_key, low, largest):
    longest = values.shape.index(max(values.shape))
    spots = []
    for shift in (0, 1):
        where = [jax.random.randint(jax.random.fold_in(stream_key, axis), (), 0, length) for axis, length in enumerate(values.shape)]
        where[longest] = (where[longest] + shift) % values.shape[longest]
        spots.append(tuple(where))
    return values.at[spots[0]].set(low).at[spots[1]].set(largest)


def block_scale(own_key, extent, cuts, low, largest):
    loudness = 1.0
    for axis_at, shards_of in cuts:
        draws = jax.random.uniform(jax.random.fold_in(jax.random.fold_in(own_key, 6), axis_at), (shards_of,), jnp.float32, low / len(cuts), largest / len(cuts))
        loudness = loudness * jnp.repeat(jnp.exp(draws), extent[axis_at] // shards_of).reshape((-1,) + (1,) * (len(extent) - 1 - axis_at))
    return loudness


def centred(rng, shape, width, limit, split=(), kind=jnp.bfloat16):
    gain = block_scale(rng, shape, split, -0.22, 0.18) if split else 1.0
    drawn = jax.random.normal(rng, shape, jnp.float32) * width * gain
    return jnp.minimum(jnp.maximum(drawn, -limit), limit).astype(kind)


def setup_inputs(seed: int = 0) -> dict:
    key_of = jax.random.split(jax.random.key(seed), 13)
    atm_flux = centred(key_of[0], (F, NA), 1.0, 6.0, ((1, 32),))
    remap_send = plant(jax.random.randint(key_of[1], (N_PATCH, SPAN, CAP), 0, ABLK), jax.random.fold_in(key_of[1], 1), 0, ABLK - 1).astype(jnp.int32)
    remap_target = plant(jax.random.randint(key_of[2], (N_PATCH, SPAN, CAP), 0, OBLK), jax.random.fold_in(key_of[2], 1), 0, OBLK - 1).astype(jnp.int32)
    remap_counts = draw_remap_counts(jax.random.fold_in(key_of[12], 71), 0)
    remap_weights = centred(key_of[4], (N_PATCH, SPAN, CAP, BLOCK, BLOCK), BLOCK ** -0.5, 0.5, ((0, 32),))
    coupling = centred(key_of[5], (NTR, F), F ** -0.5, 2.0, (), jnp.float32)
    tracer = centred(key_of[6], (NTR, LEV, NOC), 1.0, 6.0, ((2, 32),), jnp.float32)
    wet = draw_wet(jax.random.fold_in(key_of[12], 71), 0)
    mix_inverse = draw_mix_inverse(jax.random.fold_in(key_of[12], 71), 0)
    halo_send = plant(jax.random.randint(key_of[9], (N_PATCH, HSPAN, HR, BLOCK), 0, OC), jax.random.fold_in(key_of[9], 1), 0, OC - 1).astype(jnp.int32)
    halo_ghost = plant(jax.random.randint(key_of[10], (N_PATCH, HSPAN, HR, BLOCK), 0, OC), jax.random.fold_in(key_of[10], 1), 0, OC - 1).astype(jnp.int32)
    halo_rows = draw_halo_rows(jax.random.fold_in(key_of[12], 71), 0)
    return dict(atm_flux=atm_flux, remap_send=remap_send, remap_target=remap_target, remap_counts=remap_counts, remap_weights=remap_weights, coupling=coupling, tracer=tracer, wet=wet, mix_inverse=mix_inverse, halo_send=halo_send, halo_ghost=halo_ghost, halo_rows=halo_rows)


def reference(atm_flux, remap_send, remap_target, remap_counts, remap_weights, coupling, tracer, wet, mix_inverse, halo_send, halo_ghost, halo_rows):
    wetf = wet.astype(jnp.float32)
    offsets = jnp.arange(SPAN, dtype=jnp.int32) - REACH
    blocks = atm_flux.reshape(F, N_PATCH * ABLK, BLOCK)

    def receive(ocean):
        source = (ocean - offsets) % N_PATCH
        global_id = source[:, None] * ABLK + remap_send[source, jnp.arange(SPAN, dtype=jnp.int32)]
        pieces = blocks[:, global_id].astype(jnp.float32)
        in_use = (jnp.arange(CAP, dtype=jnp.int32)[None, :] < remap_counts[ocean][:, None]).astype(jnp.float32)
        contrib = jnp.einsum("fdci,dcij->dcfj", pieces, remap_weights[ocean].astype(jnp.float32), precision=lax.Precision.HIGHEST)
        contrib = contrib * in_use[:, :, None, None]
        table = (remap_target[ocean][..., None] == jnp.arange(OBLK, dtype=jnp.int32)).astype(jnp.float32)
        return jnp.einsum("dcb,dcfj->fbj", table, contrib, precision=lax.Precision.HIGHEST).reshape(F, OBLK * BLOCK)

    flux = lax.map(receive, jnp.arange(N_PATCH, dtype=jnp.int32))
    ocean_flux = jnp.transpose(flux, (1, 0, 2)).reshape(F, NOC) * wetf
    surface = jnp.dot(coupling, ocean_flux, precision=lax.Precision.HIGHEST)
    rhs = tracer.at[:, 0, :].add(surface)
    shaped = rhs.reshape(NTR, LEV, N_PATCH * OBLK, BLOCK)
    solved = jnp.einsum("blk,tkbc->tlbc", mix_inverse, shaped, precision=lax.Precision.HIGHEST).reshape(NTR, LEV, NOC)
    mixed = wetf * solved + (1.0 - wetf) * tracer
    sent = mixed.astype(jnp.bfloat16)
    halo_offsets = jnp.concatenate([jnp.arange(-REACH, 0, dtype=jnp.int32), jnp.arange(1, REACH + 1, dtype=jnp.int32)])
    ocean_ids = jnp.arange(N_PATCH, dtype=jnp.int32)[:, None]
    source = (ocean_ids - halo_offsets[None, :]) % N_PATCH
    source_cells = halo_send[source, jnp.arange(HSPAN, dtype=jnp.int32)[None, :]]
    source_glob = source[:, :, None, None] * OC + source_cells
    target_glob = ocean_ids[:, :, None, None] * OC + halo_ghost
    in_use = (jnp.arange(HR, dtype=jnp.int32)[None, None, :] < halo_rows[:, :, None]).astype(jnp.float32)
    values = sent[:, :, source_glob].astype(jnp.float32)
    current = mixed[:, :, target_glob]
    weight = in_use[..., None] * wetf[target_glob]
    increment = 0.25 * (values - current) * weight
    tracer_out = mixed.at[:, :, target_glob].add(increment)
    return ocean_flux, tracer_out
```

```python
import jax
import jax.numpy as jnp
from jax import lax
from jax.experimental import pallas as pl
from jax.experimental.pallas import tpu as pltpu
from jax.sharding import PartitionSpec as P

MESH = pl.DeviceIdType.MESH
CHUNKS = 4
EARLY = 1
TILE = 512


def split(value):
    high = value.astype(jnp.bfloat16)
    return high, (value - high.astype(jnp.float32)).astype(jnp.bfloat16)


def product(left, right):
    return jnp.dot(left, right, preferred_element_type=jnp.float32)


def couple_kernel(
    send_hbm,
    target_hbm,
    counts_hbm,
    coupling_hbm,
    halo_rows_hbm,
    atm_hbm,
    wet_hbm,
    halo_send_hbm,
    halo_ghost_hbm,
    weights_hbm,
    tracer_hbm,
    inverse_hbm,
    flux_out,
    mixed,
    values,
    scatter,
    remap_send,
    remap_target,
    remap_counts,
    coupling,
    halo_rows,
    picks_smem,
    atm,
    atm_blocks,
    wet,
    halo_send,
    halo_ghost,
    weights,
    tracer,
    inverse,
    base_rows,
    gathered,
    surface,
    surface_rows,
    surface_gathered,
    surface_out,
    surface_in,
    total,
    outgoing,
    arrived,
    picked,
    received,
    column,
    tips,
    tips_in,
    cells_in,
    load_sem,
    small_sem,
    flux_send_sem,
    flux_recv_sem,
    halo_send_sem,
    halo_recv_sem,
    side_send_sem,
    side_recv_sem,
):
    size = lax.axis_size("patch")
    me = lax.axis_index("patch")
    spans, slots = remap_send.shape[0], remap_send.shape[2]
    radius = spans // 2
    tracers, levels, cells = tracer.shape
    block = weights.shape[-1]
    blocks = cells // block
    fluxes = atm.shape[0]
    steps = [d - radius for d in range(spans) if d != radius]
    hosts = len(steps)
    depth, lanes = halo_send.shape[1], halo_send.shape[2]
    picks = depth * lanes

    def peer(step):
        return lax.rem(me + step + size, size)
    barrier = pltpu.get_barrier_semaphore()
    for step in steps:
        pl.semaphore_signal(barrier, inc=1, device_id=(peer(step),), device_id_type=MESH)

    small = [
        pltpu.make_async_copy(src, dst, small_sem.at[i])
        for i, (src, dst) in enumerate(
            [
                (send_hbm, remap_send),
                (atm_hbm, atm),
                (wet_hbm, wet),
                (target_hbm, remap_target),
                (counts_hbm, remap_counts),
                (coupling_hbm, coupling),
                (halo_rows_hbm, halo_rows),
                (halo_send_hbm.at[0], picks_smem),
                (halo_send_hbm.at[0], halo_send),
                (halo_ghost_hbm.at[0], halo_ghost),
            ]
        )
    ]
    for copy in small:
        copy.start()
    part, span = blocks // CHUNKS, cells // CHUNKS
    loads = []
    for chunk in range(CHUNKS):
        run = pl.ds(chunk * span, span)
        group = pl.ds(chunk * part, part)
        loads.append(
            pltpu.make_async_copy(inverse_hbm.at[group], inverse.at[group], load_sem.at[2 * chunk])
        )
        loads.append(
            pltpu.make_async_copy(
                tracer_hbm.at[:, :, run], tracer.at[:, :, run], load_sem.at[2 * chunk + 1]
            )
        )
    for load in loads:
        load.start()
    weight_load = pltpu.make_async_copy(weights_hbm.at[0], weights, load_sem.at[2 * CHUNKS])
    weight_load.start()
    for copy in small[:2]:
        copy.wait()
    for a in range(atm_blocks.shape[0]):
        atm_blocks[a] = atm[:, a * block : (a + 1) * block]
    for d in range(spans):
        for c in range(slots):
            piece = atm_blocks[remap_send[d, 0, c]]
            if d == radius:
                arrived[d, c] = piece
            else:
                outgoing[d, c] = piece

    lane = lax.broadcasted_iota(jnp.int32, (levels, block), 1)

    def mix_block(k):
        run = slice(k * block, (k + 1) * block)
        full = inverse[k]
        high, low = split(full)
        awake = wet[0:1, run] != 0
        held = [tracer[t, :, run] for t in range(tracers)]
        right_high, right_low = split(jnp.concatenate(held, axis=1))
        solved = product(
            jnp.concatenate([high, low, high], axis=1),
            jnp.concatenate([right_high, right_high, right_low], axis=0),
        )
        for t in range(tracers):
            value = jnp.where(awake, solved[:, t * block : (t + 1) * block], held[t])
            mixed[t, :, run] = value
            base_rows[t, run, :] = jnp.transpose(value)
        first = jnp.broadcast_to(full[:, 0:1], (levels, block))
        if k % block == 0:
            column[k // block] = first
        else:
            column[k // block] = jnp.where(lane == k % block, first, column[k // block])

    def mix_chunk(chunk):
        loads[2 * chunk].wait()
        loads[2 * chunk + 1].wait()
        for k in range(chunk * part, (chunk + 1) * part):
            mix_block(k)
    small[2].wait()
    for chunk in range(EARLY):
        mix_chunk(chunk)
    pl.semaphore_wait(barrier, len(steps))
    flux_copies = {}
    for step in sorted(steps, key=lambda step: -abs(step)):
        d = step + radius
        flux_copies[d] = pltpu.make_async_remote_copy(
            src_ref=outgoing.at[d],
            dst_ref=arrived.at[d],
            send_sem=flux_send_sem.at[d],
            recv_sem=flux_recv_sem.at[d],
            device_id=(peer(step),),
            device_id_type=MESH,
        )
        flux_copies[d].start()
    for chunk in range(EARLY, CHUNKS):
        mix_chunk(chunk)

    order = [h for h in range(hosts) if steps[h] > 0]
    order += [h for h in range(hosts)[::-1] if steps[h] < 0]

    def remote(source, target, sems, h):
        return pltpu.make_async_remote_copy(
            src_ref=source,
            dst_ref=target.at[h],
            send_sem=sems[0].at[h],
            recv_sem=sems[1].at[h],
            device_id=(peer(steps[h]),),
            device_id_type=MESH,
        )
    for copy in small[3:]:
        copy.wait()
    halo_copies = []
    for h in order:
        for row in range(picks):
            cell = picks_smem[h, row // lanes, row % lanes]
            for t in range(tracers):
                gathered[t, row] = base_rows[t, cell]
        for t in range(tracers):
            picked[h, t * levels : (t + 1) * levels, :] = jnp.transpose(gathered[t]).astype(
                jnp.bfloat16
            )
        copy = remote(picked.at[h], received, (halo_send_sem, halo_recv_sem), h)
        copy.start()
        halo_copies.append(copy)
    flat = jnp.concatenate([jnp.transpose(column[i]) for i in range(column.shape[0])], axis=0)
    tips[...] = flat[:blocks].astype(jnp.bfloat16)
    for h in order:
        for source, target, kind in ((tips, tips_in, 0), (halo_send.at[h], cells_in, 1)):
            copy = remote(source, target, (side_send_sem.at[kind], side_recv_sem.at[kind]), h)
            copy.start()
            halo_copies.append(copy)
    weight_load.wait()
    owner = lax.broadcasted_iota(jnp.int32, (blocks, fluxes, block), 0)
    blank = jnp.zeros((fluxes, block), jnp.int32)
    for copy in flux_copies.values():
        copy.wait_recv()
    for d in range(spans):
        pieces = []
        for c in range(slots):
            used = (blank + remap_counts[0, d]) > c
            piece = jnp.where(used, arrived[d, c].astype(jnp.float32), 0.0)
            placed = jnp.where(owner == remap_target[d, 0, c], piece[None], 0.0)
            pieces.append(placed.reshape(blocks * fluxes, block).astype(jnp.bfloat16))
        left = jnp.concatenate(pieces, axis=1)
        term = product(left, weights[d].reshape(slots * block, block))
        if d == 0:
            total[...] = term
        else:
            total[...] += term
    pad = surface.shape[0] - tracers
    for b in range(blocks):
        run = slice(b * block, (b + 1) * block)
        flux = total[b * fluxes : (b + 1) * fluxes, :] * wet[0:1, run].astype(jnp.float32)
        flux_out[:, run] = flux
        rows = []
        for t in range(tracers):
            value = coupling[t, 0] * flux[0:1, :]
            for f in range(1, fluxes):
                value = value + coupling[t, f] * flux[f : f + 1, :]
            rows.append(value)
        stacked = jnp.concatenate(rows + [jnp.zeros((pad, block), jnp.float32)], axis=0)
        surface[:, run] = stacked
        surface_rows[run, :] = jnp.transpose(stacked)
    for h in order:
        for row in range(picks):
            cell = picks_smem[h, row // lanes, row % lanes]
            surface_gathered[row] = surface_rows[cell]
        surface_out[h] = jnp.transpose(surface_gathered[...])[:tracers]
        copy = remote(surface_out.at[h], surface_in, (side_send_sem.at[2], side_recv_sem.at[2]), h)
        copy.start()
        halo_copies.append(copy)
    ghosts = []
    line = jnp.zeros((1, lanes), jnp.int32)
    for h in range(hosts):
        for r in range(depth):
            used = (line + halo_rows[0, h]) > r
            ghosts.append(jnp.where(used, halo_ghost[h, r : r + 1, :], -1))
    places = jnp.transpose(jnp.concatenate(ghosts, axis=0))
    ones = jnp.ones((16, len(ghosts) * lanes), jnp.bfloat16)
    rows = min(TILE, cells)

    def scatter_cells(index, _):
        base = pl.multiple_of(index * rows, rows)
        run = pl.ds(base, rows)
        ids = lax.broadcasted_iota(jnp.int32, (lanes, rows), 1) + base
        pull = 0.25 * wet[0:1, run].astype(jnp.float32)
        for i in range(len(ghosts)):
            hit = ids == places[:, i : i + 1]
            scatter[i * lanes : (i + 1) * lanes, run] = jnp.where(hit, pull, 0.0).astype(
                jnp.bfloat16
            )
        keep = 1.0 - product(ones, scatter[:, run])[0:1]
        for i in range(rows // block):
            near = pl.ds(pl.multiple_of(base + i * block, block), block)
            first = jnp.broadcast_to(
                inverse[index * (rows // block) + i, :, 0:1], (levels, block)
            )
            for t in range(tracers):
                mixed[t, :, near] = keep[:, i * block : (i + 1) * block] * (
                    mixed[t, :, near] + first * surface[t : t + 1, near]
                )
        return 0
    lax.fori_loop(0, cells // rows, scatter_cells, 0)

    ids = lax.broadcasted_iota(jnp.int32, (blocks, picks), 0)
    shift = block.bit_length() - 1

    def correct(h):
        for source, target, sems in (
            (picked.at[h], received, (halo_send_sem, halo_recv_sem)),
            (tips, tips_in, (side_send_sem.at[0], side_recv_sem.at[0])),
            (halo_send.at[h], cells_in, (side_send_sem.at[1], side_recv_sem.at[1])),
            (surface_out.at[h], surface_in, (side_send_sem.at[2], side_recv_sem.at[2])),
        ):
            remote(source, target, sems, h).wait_recv()
        where = jnp.concatenate([cells_in[h, r : r + 1, :] for r in range(depth)], axis=1)
        hit = ids == lax.shift_right_logical(where, shift)
        first = lax.dot_general(
            tips_in[h],
            jnp.where(hit, 1.0, 0.0).astype(jnp.bfloat16),
            (((0,), (0,)), ((), ())),
            preferred_element_type=jnp.float32,
        )
        for t in range(tracers):
            level = slice(t * levels, (t + 1) * levels)
            value = received[h, level, :].astype(jnp.float32) + first * surface_in[h, t : t + 1, :]
            values[h, level, :] = value.astype(jnp.bfloat16)

    half = hosts // 2
    for h in range(half)[::-1]:
        correct(h)

    left = jnp.concatenate([values[h] for h in range(half)], axis=1)
    for index in range(cells // rows):
        run = slice(index * rows, (index + 1) * rows)
        summed = product(left, scatter[: half * picks, run])
        for t in range(tracers):
            mixed[t, :, run] += summed[t * levels : (t + 1) * levels]
    for h in range(half, hosts):
        correct(h)
    for copy in list(flux_copies.values()) + halo_copies:
        copy.wait_send()


def halo_kernel(values, scatter, kept, flux_in, flux_out, out):
    tracers, levels, tile = out.shape
    hosts, _, picks = values.shape
    half = hosts // 2
    run = pl.ds(pl.multiple_of(pl.program_id(0) * tile, tile), tile)
    left = jnp.concatenate([values[h] for h in range(half, hosts)], axis=1)
    summed = product(left, scatter[half * picks :, run])
    for t in range(tracers):
        out[t] = kept[t, :, run] + summed[t * levels : (t + 1) * levels]
    flux_out[...] = flux_in[...]


def body(
    atm_flux,
    remap_send,
    remap_target,
    remap_counts,
    remap_weights,
    coupling,
    tracer,
    wet,
    mix_inverse,
    halo_send,
    halo_ghost,
    halo_rows,
):
    spans, slots = remap_send.shape[1:]
    block = remap_weights.shape[-1]
    fluxes = atm_flux.shape[0]
    tracers, levels, cells = tracer.shape
    blocks = cells // block
    hosts, depth, lanes = halo_send.shape[1:]
    picks = depth * lanes
    features = tracers * levels
    lead = -(-tracers // 8) * 8
    vmem = pl.BlockSpec(memory_space=pltpu.VMEM)
    hbm = pl.BlockSpec(memory_space=pltpu.HBM)
    dma = pltpu.SemaphoreType.DMA
    flux, kept, values, scatter = pl.pallas_call(
        couple_kernel,
        out_shape=(
            pltpu.VMEM((fluxes, cells), jnp.float32),
            pltpu.VMEM((tracers, levels, cells), jnp.float32),
            pltpu.VMEM((hosts, features, picks), jnp.bfloat16),
            pltpu.VMEM((hosts * picks, cells), jnp.bfloat16),
        ),
        in_specs=[hbm] * 12,
        out_specs=(vmem, vmem, vmem, vmem),
        scratch_shapes=[
            pltpu.SMEM((spans, 1, slots), jnp.int32),
            pltpu.SMEM((spans, 1, slots), jnp.int32),
            pltpu.SMEM((1, spans), jnp.int32),
            pltpu.SMEM((tracers, fluxes), jnp.float32),
            pltpu.SMEM((1, hosts), jnp.int32),
            pltpu.SMEM((hosts, depth, lanes), jnp.int32),
            pltpu.VMEM(atm_flux.shape, jnp.bfloat16),
            pltpu.VMEM((atm_flux.shape[1] // block, fluxes, block), jnp.bfloat16),
            pltpu.VMEM((1, cells), jnp.int32),
            pltpu.VMEM((hosts, depth, lanes), jnp.int32),
            pltpu.VMEM((hosts, depth, lanes), jnp.int32),
            pltpu.VMEM((spans, slots, block, block), jnp.bfloat16),
            pltpu.VMEM((tracers, levels, cells), jnp.float32),
            pltpu.VMEM((blocks, levels, levels), jnp.float32),
            pltpu.VMEM((tracers, cells, levels), jnp.float32),
            pltpu.VMEM((tracers, picks, levels), jnp.float32),
            pltpu.VMEM((lead, cells), jnp.float32),
            pltpu.VMEM((cells, lead), jnp.float32),
            pltpu.VMEM((picks, lead), jnp.float32),
            pltpu.VMEM((hosts, tracers, picks), jnp.float32),
            pltpu.VMEM((hosts, tracers, picks), jnp.float32),
            pltpu.VMEM((blocks * fluxes, block), jnp.float32),
            pltpu.VMEM((spans, slots, fluxes, block), jnp.bfloat16),
            pltpu.VMEM((spans, slots, fluxes, block), jnp.bfloat16),
            pltpu.VMEM((hosts, features, picks), jnp.bfloat16),
            pltpu.VMEM((hosts, features, picks), jnp.bfloat16),
            pltpu.VMEM((-(-blocks // block), levels, block), jnp.float32),
            pltpu.VMEM((blocks, levels), jnp.bfloat16),
            pltpu.VMEM((hosts, blocks, levels), jnp.bfloat16),
            pltpu.VMEM((hosts, depth, lanes), jnp.int32),
            dma((2 * CHUNKS + 1,)),
            dma((10,)),
            dma((spans,)),
            dma((spans,)),
            dma((hosts,)),
            dma((hosts,)),
            dma((3, hosts)),
            dma((3, hosts)),
        ],
        compiler_params=pltpu.CompilerParams(
            collective_id=0, has_side_effects=True, vmem_limit_bytes=48 * 1024 * 1024
        ),
        name="couple",
    )(
        remap_send.transpose(1, 0, 2),
        remap_target.transpose(1, 0, 2),
        remap_counts,
        coupling,
        halo_rows,
        atm_flux,
        wet.reshape(1, cells),
        halo_send,
        halo_ghost,
        remap_weights,
        tracer,
        mix_inverse,
    )
    tile = min(TILE, cells)
    return pl.pallas_call(
        halo_kernel,
        grid=(cells // tile,),
        out_shape=(
            jax.ShapeDtypeStruct((fluxes, cells), jnp.float32),
            jax.ShapeDtypeStruct((tracers, levels, cells), jnp.float32),
        ),
        in_specs=[vmem, vmem, vmem, pl.BlockSpec((fluxes, tile), lambda i: (0, i))],
        out_specs=(
            pl.BlockSpec((fluxes, tile), lambda i: (0, i)),
            pl.BlockSpec((tracers, levels, tile), lambda i: (0, 0, i)),
        ),
        compiler_params=pltpu.CompilerParams(vmem_limit_bytes=32 * 1024 * 1024),
        name="halo",
    )(values, scatter, kept, flux)


def solution(mesh):
    return jax.shard_map(
        body,
        mesh=mesh,
        in_specs=(
            P(None, "patch"),
            P("patch", None, None),
            P("patch", None, None),
            P("patch", None),
            P("patch", None, None, None, None),
            P(),
            P(None, None, "patch"),
            P("patch"),
            P("patch", None, None),
            P("patch", None, None, None),
            P("patch", None, None, None),
            P("patch", None),
        ),
        out_specs=(P(None, "patch"), P(None, None, "patch")),
        check_vma=False,
    )
```

```python
import jax
import jax.numpy as jnp
from jax import lax
from jax.experimental import pallas as pl
from jax.experimental.pallas import tpu as pltpu
from jax.sharding import PartitionSpec as P

MESH = pl.DeviceIdType.MESH
CHUNKS = 4
TILE = 512


def split(value):
    high = value.astype(jnp.bfloat16)
    return high, (value - high.astype(jnp.float32)).astype(jnp.bfloat16)


def product(left, right):
    return jnp.dot(left, right, preferred_element_type=jnp.float32)


def couple_kernel(
    send_hbm,
    target_hbm,
    counts_hbm,
    coupling_hbm,
    halo_rows_hbm,
    atm_hbm,
    wet_hbm,
    halo_send_hbm,
    halo_ghost_hbm,
    weights_hbm,
    tracer_hbm,
    inverse_hbm,
    flux_out,
    mixed,
    values,
    scatter,
    remap_send,
    remap_target,
    remap_counts,
    coupling,
    halo_rows,
    picks_smem,
    atm,
    atm_blocks,
    wet,
    halo_send,
    halo_ghost,
    weights,
    tracer,
    inverse,
    base_rows,
    gathered,
    factor,
    keep,
    surface,
    surface_rows,
    surface_gathered,
    surface_out,
    surface_in,
    total,
    outgoing,
    arrived,
    picked,
    received,
    column,
    tips,
    tips_in,
    cells_in,
    load_sem,
    small_sem,
    flux_send_sem,
    flux_recv_sem,
    halo_send_sem,
    halo_recv_sem,
    side_send_sem,
    side_recv_sem,
):
    size = lax.axis_size("patch")
    me = lax.axis_index("patch")
    spans, slots = remap_send.shape[0], remap_send.shape[2]
    radius = spans // 2
    tracers, levels, cells = tracer.shape
    block = weights.shape[-1]
    blocks = cells // block
    fluxes = atm.shape[0]
    steps = [d - radius for d in range(spans) if d != radius]
    hosts = len(steps)
    depth, lanes = halo_send.shape[1], halo_send.shape[2]
    picks = depth * lanes

    def peer(step):
        return lax.rem(me + step + size, size)
    barrier = pltpu.get_barrier_semaphore()
    for step in steps:
        pl.semaphore_signal(barrier, inc=1, device_id=(peer(step),), device_id_type=MESH)

    small = [
        pltpu.make_async_copy(src, dst, small_sem.at[i])
        for i, (src, dst) in enumerate(
            [
                (send_hbm, remap_send),
                (atm_hbm, atm),
                (wet_hbm, wet),
                (target_hbm, remap_target),
                (counts_hbm, remap_counts),
                (coupling_hbm, coupling),
                (halo_rows_hbm, halo_rows),
                (halo_send_hbm.at[0], picks_smem),
                (halo_send_hbm.at[0], halo_send),
                (halo_ghost_hbm.at[0], halo_ghost),
            ]
        )
    ]
    for copy in small:
        copy.start()
    part, span = blocks // CHUNKS, cells // CHUNKS
    loads = {}
    for t in range(tracers):
        for chunk in range(CHUNKS):
            run = pl.ds(chunk * span, span)
            bunch = pl.ds(chunk * part, part)
            if t == 0:
                loads[chunk] = pltpu.make_async_copy(
                    inverse_hbm.at[bunch], inverse.at[bunch], load_sem.at[chunk]
                )
                loads[chunk].start()
            loads[t, chunk] = pltpu.make_async_copy(
                tracer_hbm.at[t, :, run],
                tracer.at[t, :, run],
                load_sem.at[(1 + t) * CHUNKS + chunk],
            )
            loads[t, chunk].start()
    weight_load = pltpu.make_async_copy(weights_hbm.at[0], weights, load_sem.at[(1 + tracers) * CHUNKS])
    weight_load.start()
    for copy in small[:2]:
        copy.wait()
    for a in range(atm_blocks.shape[0]):
        atm_blocks[a] = atm[:, a * block : (a + 1) * block]
    for d in range(spans):
        for c in range(slots):
            piece = atm_blocks[remap_send[d, 0, c]]
            if d == radius:
                arrived[d, c] = piece
            else:
                outgoing[d, c] = piece

    low = me < radius
    order = [h for h in range(hosts) if steps[h] > 0]
    order += [h for h in range(hosts)[::-1] if steps[h] < 0]

    def remote(source, target, sems, index, h):
        return pltpu.make_async_remote_copy(
            src_ref=source,
            dst_ref=target,
            send_sem=sems[0].at[index],
            recv_sem=sems[1].at[index],
            device_id=(peer(steps[h]),),
            device_id_type=MESH,
        )

    def flux_copy(h):
        d = steps[h] + radius
        return remote(outgoing.at[d], arrived.at[d], (flux_send_sem, flux_recv_sem), h, h)

    def row_copy(h, t):
        level = pl.ds(t * levels, levels)
        return remote(
            picked.at[h, level], received.at[h, level], (halo_send_sem, halo_recv_sem), (h, t), h
        )

    def side_copy(h, kind):
        source, target = (
            (tips, tips_in.at[h]),
            (halo_send.at[h], cells_in.at[h]),
            (surface_out.at[h], surface_in.at[h]),
        )[kind]
        return remote(source, target, (side_send_sem, side_recv_sem), (kind, h), h)

    def enter():
        pl.semaphore_wait(barrier, len(steps))
        for h in sorted(range(hosts), key=lambda h: -abs(steps[h])):
            flux_copy(h).start()

    lane = lax.broadcasted_iota(jnp.int32, (levels, block), 1)

    def mix_block(k, t):
        run = slice(k * block, (k + 1) * block)
        if t == 0:
            full = inverse[k]
            high, low_part = split(full)
            left = jnp.concatenate([high, low_part, high], axis=1)
            factor[k] = left
            first = jnp.broadcast_to(full[:, 0:1], (levels, block))
            if k % block == 0:
                column[k // block] = first
            else:
                column[k // block] = jnp.where(lane == k % block, first, column[k // block])
        else:
            left = factor[k]
        held = tracer[t, :, run]
        right_high, right_low = split(held)
        solved = product(left, jnp.concatenate([right_high, right_high, right_low], axis=0))
        value = jnp.where(wet[0:1, run] != 0, solved, held)
        mixed[t, :, run] = value
        base_rows[t, run, :] = jnp.transpose(value)

    def mix_chunk(chunk, t):
        if t == 0:
            loads[chunk].wait()
        loads[t, chunk].wait()
        for k in range(chunk * part, (chunk + 1) * part):
            mix_block(k, t)
    small[2].wait()
    mix_chunk(0, 0)

    @pl.when(jnp.logical_not(low))
    def _():
        enter()

    for chunk in range(1, CHUNKS):
        mix_chunk(chunk, 0)
    for copy in small[3:]:
        copy.wait()
    held_back = [(h, tracers - 1) for h in order if steps[h] < 0]
    flat = jnp.concatenate([jnp.transpose(column[i]) for i in range(column.shape[0])], axis=0)
    tips[...] = flat[:blocks].astype(jnp.bfloat16)
    sent = []
    for t in range(tracers):
        if t > 0:
            for chunk in range(CHUNKS):
                mix_chunk(chunk, t)
        for h in order:
            for row in range(picks):
                cell = picks_smem[h, row // lanes, row % lanes]
                gathered[row] = base_rows[t, cell]
            picked[h, t * levels : (t + 1) * levels, :] = jnp.transpose(gathered[...]).astype(
                jnp.bfloat16
            )
            bundle = [row_copy(h, t)] if (h, t) not in held_back else []
            if t == 0:
                bundle += [side_copy(h, 0), side_copy(h, 1)]
            sent += bundle

            @pl.when(jnp.logical_not(low))
            def _():
                for copy in bundle:
                    copy.start()

    @pl.when(low)
    def _():
        enter()
        for copy in sent:
            copy.start()
    ghosts = []
    line = jnp.zeros((1, lanes), jnp.int32)
    for h in range(hosts):
        for r in range(depth):
            used = (line + halo_rows[0, h]) > r
            ghosts.append(jnp.where(used, halo_ghost[h, r : r + 1, :], -1))
    places = jnp.transpose(jnp.concatenate(ghosts, axis=0))
    rows = min(TILE, cells)
    ones = jnp.ones((16, len(ghosts) * lanes), jnp.bfloat16)
    marks = [
        jnp.broadcast_to(places[:, i : i + 1], (lanes, rows)).astype(jnp.int16)
        for i in range(len(ghosts))
    ]
    ids = lax.broadcasted_iota(jnp.int32, (lanes, rows), 1).astype(jnp.int16)
    for index in range(cells // rows):
        run = slice(index * rows, (index + 1) * rows)
        pull = jnp.broadcast_to(0.25 * wet[0:1, run].astype(jnp.float32), (lanes, rows)).astype(
            jnp.bfloat16
        )
        here = ids + jnp.int16(index * rows)
        for i in range(len(ghosts)):
            scatter[i * lanes : (i + 1) * lanes, run] = jnp.where(
                here == marks[i], pull, jnp.bfloat16(0)
            )
        keep[:, run] = 1.0 - product(ones, scatter[:, run])[0:1]
    weight_load.wait()
    owner = lax.broadcasted_iota(jnp.int32, (blocks, fluxes, block), 0)
    blank = jnp.zeros((fluxes, block), jnp.int32)
    for h in range(hosts):
        flux_copy(h).wait_recv()
    for d in range(spans):
        pieces = []
        for c in range(slots):
            used = (blank + remap_counts[0, d]) > c
            piece = jnp.where(used, arrived[d, c].astype(jnp.float32), 0.0)
            placed = jnp.where(owner == remap_target[d, 0, c], piece[None], 0.0)
            pieces.append(placed.reshape(blocks * fluxes, block).astype(jnp.bfloat16))
        left = jnp.concatenate(pieces, axis=1)
        term = product(left, weights[d].reshape(slots * block, block))
        if d == 0:
            total[...] = term
        else:
            total[...] += term
    pad = surface.shape[0] - tracers
    for b in range(blocks):
        run = slice(b * block, (b + 1) * block)
        flux = total[b * fluxes : (b + 1) * fluxes, :] * wet[0:1, run].astype(jnp.float32)
        flux_out[:, run] = flux
        rows = []
        for t in range(tracers):
            value = coupling[t, 0] * flux[0:1, :]
            for f in range(1, fluxes):
                value = value + coupling[t, f] * flux[f : f + 1, :]
            rows.append(value)
        stacked = jnp.concatenate(rows + [jnp.zeros((pad, block), jnp.float32)], axis=0)
        surface[:, run] = stacked
        surface_rows[run, :] = jnp.transpose(stacked)
    for h in order:
        for row in range(picks):
            cell = picks_smem[h, row // lanes, row % lanes]
            surface_gathered[row] = surface_rows[cell]
        surface_out[h] = jnp.transpose(surface_gathered[...])[:tracers]
        side_copy(h, 2).start()
    for h, t in held_back:
        row_copy(h, t).start()
    for k in range(blocks):
        run = slice(k * block, (k + 1) * block)
        first = jnp.broadcast_to(inverse[k, :, 0:1], (levels, block))
        for t in range(tracers):
            mixed[t, :, run] = keep[:, run] * (
                mixed[t, :, run] + first * surface[t : t + 1, run]
            )

    ids = lax.broadcasted_iota(jnp.int32, (blocks, picks), 0)
    shift = block.bit_length() - 1

    def correct(h):
        for kind in range(3):
            side_copy(h, kind).wait_recv()
        for t in range(tracers):
            row_copy(h, t).wait_recv()
        where = jnp.concatenate([cells_in[h, r : r + 1, :] for r in range(depth)], axis=1)
        hit = ids == lax.shift_right_logical(where, shift)
        first = lax.dot_general(
            tips_in[h],
            jnp.where(hit, 1.0, 0.0).astype(jnp.bfloat16),
            (((0,), (0,)), ((), ())),
            preferred_element_type=jnp.float32,
        )
        for t in range(tracers):
            level = slice(t * levels, (t + 1) * levels)
            value = received[h, level, :].astype(jnp.float32) + first * surface_in[h, t : t + 1, :]
            values[level, h * picks : (h + 1) * picks] = value.astype(jnp.bfloat16)

    for h in order:
        correct(h)
    for h in range(hosts):
        flux_copy(h).wait_send()
        for t in range(tracers):
            row_copy(h, t).wait_send()
        for kind in range(3):
            side_copy(h, kind).wait_send()


def halo_kernel(values, scatter, kept, flux_in, flux_out, out, stage, sems):
    tracers, levels, cells = out.shape
    flux_copy = pltpu.make_async_copy(flux_in, flux_out, sems.at[0])
    flux_copy.start()
    tile = min(TILE, cells)
    copies = [flux_copy]
    for index in range(cells // tile):
        run = slice(index * tile, (index + 1) * tile)
        summed = product(values[...], scatter[:, run])
        for t in range(tracers):
            stage[t, :, run] = kept[t, :, run] + summed[t * levels : (t + 1) * levels]
        area = pl.ds(index * tile, tile)
        copy = pltpu.make_async_copy(
            stage.at[:, :, area], out.at[:, :, area], sems.at[1 + index]
        )
        copy.start()
        copies.append(copy)
    for copy in copies:
        copy.wait()


def body(
    atm_flux,
    remap_send,
    remap_target,
    remap_counts,
    remap_weights,
    coupling,
    tracer,
    wet,
    mix_inverse,
    halo_send,
    halo_ghost,
    halo_rows,
):
    spans, slots = remap_send.shape[1:]
    block = remap_weights.shape[-1]
    fluxes = atm_flux.shape[0]
    tracers, levels, cells = tracer.shape
    blocks = cells // block
    hosts, depth, lanes = halo_send.shape[1:]
    picks = depth * lanes
    features = tracers * levels
    lead = -(-tracers // 8) * 8
    vmem = pl.BlockSpec(memory_space=pltpu.VMEM)
    hbm = pl.BlockSpec(memory_space=pltpu.HBM)
    dma = pltpu.SemaphoreType.DMA
    flux, kept, values, scatter = pl.pallas_call(
        couple_kernel,
        out_shape=(
            pltpu.VMEM((fluxes, cells), jnp.float32),
            pltpu.VMEM((tracers, levels, cells), jnp.float32),
            pltpu.VMEM((features, hosts * picks), jnp.bfloat16),
            pltpu.VMEM((hosts * picks, cells), jnp.bfloat16),
        ),
        in_specs=[hbm] * 12,
        out_specs=(vmem, vmem, vmem, vmem),
        scratch_shapes=[
            pltpu.SMEM((spans, 1, slots), jnp.int32),
            pltpu.SMEM((spans, 1, slots), jnp.int32),
            pltpu.SMEM((1, spans), jnp.int32),
            pltpu.SMEM((tracers, fluxes), jnp.float32),
            pltpu.SMEM((1, hosts), jnp.int32),
            pltpu.SMEM((hosts, depth, lanes), jnp.int32),
            pltpu.VMEM(atm_flux.shape, jnp.bfloat16),
            pltpu.VMEM((atm_flux.shape[1] // block, fluxes, block), jnp.bfloat16),
            pltpu.VMEM((1, cells), jnp.int32),
            pltpu.VMEM((hosts, depth, lanes), jnp.int32),
            pltpu.VMEM((hosts, depth, lanes), jnp.int32),
            pltpu.VMEM((spans, slots, block, block), jnp.bfloat16),
            pltpu.VMEM((tracers, levels, cells), jnp.float32),
            pltpu.VMEM((blocks, levels, levels), jnp.float32),
            pltpu.VMEM((tracers, cells, levels), jnp.float32),
            pltpu.VMEM((picks, levels), jnp.float32),
            pltpu.VMEM((blocks, levels, 3 * levels), jnp.bfloat16),
            pltpu.VMEM((1, cells), jnp.float32),
            pltpu.VMEM((lead, cells), jnp.float32),
            pltpu.VMEM((cells, lead), jnp.float32),
            pltpu.VMEM((picks, lead), jnp.float32),
            pltpu.VMEM((hosts, tracers, picks), jnp.float32),
            pltpu.VMEM((hosts, tracers, picks), jnp.float32),
            pltpu.VMEM((blocks * fluxes, block), jnp.float32),
            pltpu.VMEM((spans, slots, fluxes, block), jnp.bfloat16),
            pltpu.VMEM((spans, slots, fluxes, block), jnp.bfloat16),
            pltpu.VMEM((hosts, features, picks), jnp.bfloat16),
            pltpu.VMEM((hosts, features, picks), jnp.bfloat16),
            pltpu.VMEM((-(-blocks // block), levels, block), jnp.float32),
            pltpu.VMEM((blocks, levels), jnp.bfloat16),
            pltpu.VMEM((hosts, blocks, levels), jnp.bfloat16),
            pltpu.VMEM((hosts, depth, lanes), jnp.int32),
            dma(((1 + tracers) * CHUNKS + 1,)),
            dma((10,)),
            dma((hosts,)),
            dma((hosts,)),
            dma((hosts, tracers)),
            dma((hosts, tracers)),
            dma((3, hosts)),
            dma((3, hosts)),
        ],
        compiler_params=pltpu.CompilerParams(
            collective_id=0, has_side_effects=True, vmem_limit_bytes=48 * 1024 * 1024
        ),
        name="couple",
    )(
        remap_send.transpose(1, 0, 2),
        remap_target.transpose(1, 0, 2),
        remap_counts,
        coupling,
        halo_rows,
        atm_flux,
        wet.reshape(1, cells),
        halo_send,
        halo_ghost,
        remap_weights,
        tracer,
        mix_inverse,
    )
    tile = min(TILE, cells)
    return pl.pallas_call(
        halo_kernel,
        out_shape=(
            jax.ShapeDtypeStruct((fluxes, cells), jnp.float32),
            jax.ShapeDtypeStruct((tracers, levels, cells), jnp.float32),
        ),
        in_specs=[vmem] * 4,
        out_specs=(hbm, hbm),
        scratch_shapes=[
            pltpu.VMEM((tracers, levels, cells), jnp.float32),
            dma((1 + cells // tile,)),
        ],
        compiler_params=pltpu.CompilerParams(vmem_limit_bytes=24 * 1024 * 1024),
        name="halo",
    )(values, scatter, kept, flux)


def solution(mesh):
    return jax.shard_map(
        body,
        mesh=mesh,
        in_specs=(
            P(None, "patch"),
            P("patch", None, None),
            P("patch", None, None),
            P("patch", None),
            P("patch", None, None, None, None),
            P(),
            P(None, None, "patch"),
            P("patch"),
            P("patch", None, None),
            P("patch", None, None, None),
            P("patch", None, None, None),
            P("patch", None),
        ),
        out_specs=(P(None, "patch"), P(None, None, "patch")),
        check_vma=False,
    )
```

```python
import functools

import jax
import jax.numpy as jnp
from jax import lax
from jax.experimental import pallas as pl
from jax.experimental.pallas import tpu as pltpu
from jax.sharding import PartitionSpec as P

MESH = pl.DeviceIdType.MESH
CHUNKS = 2
TILE = 512


def split(value):
    high = value.astype(jnp.bfloat16)
    return high, (value - high.astype(jnp.float32)).astype(jnp.bfloat16)


def product(left, right):
    return jnp.dot(left, right, preferred_element_type=jnp.float32)


def couple_kernel(
    send_hbm,
    target_hbm,
    counts_hbm,
    coupling_hbm,
    halo_rows_hbm,
    atm_hbm,
    wet_hbm,
    halo_send_hbm,
    halo_ghost_hbm,
    weights_hbm,
    tracer_hbm,
    inverse_hbm,
    flux_out,
    mixed,
    values,
    scatter,
    remap_send,
    remap_target,
    remap_counts,
    coupling,
    halo_rows,
    picks_smem,
    atm,
    atm_blocks,
    wet,
    halo_send,
    halo_ghost,
    weights,
    tracer,
    inverse,
    base_rows,
    gathered,
    early_values,
    factor,
    keep,
    surface,
    surface_rows,
    surface_gathered,
    surface_out,
    surface_in,
    total,
    outgoing,
    arrived,
    picked,
    received,
    column,
    tips,
    tips_in,
    cells_in,
    load_sem,
    small_sem,
    flux_send_sem,
    flux_recv_sem,
    halo_send_sem,
    halo_recv_sem,
    side_send_sem,
    side_recv_sem,
    ready,
):
    size = lax.axis_size("patch")
    me = lax.axis_index("patch")
    spans, slots = remap_send.shape[0], remap_send.shape[2]
    radius = spans // 2
    tracers, levels, cells = tracer.shape
    block = weights.shape[-1]
    blocks = cells // block
    fluxes = atm.shape[0]
    steps = [d - radius for d in range(spans) if d != radius]
    hosts = len(steps)
    depth, lanes = halo_send.shape[1], halo_send.shape[2]
    picks = depth * lanes

    def peer(step):
        return lax.rem(me + step + size, size)
    barrier = pltpu.get_barrier_semaphore()
    for step in steps:
        pl.semaphore_signal(barrier, inc=1, device_id=(peer(step),), device_id_type=MESH)

    small = [
        pltpu.make_async_copy(src, dst, small_sem.at[i])
        for i, (src, dst) in enumerate(
            [
                (send_hbm, remap_send),
                (atm_hbm, atm),
                (wet_hbm, wet),
                (target_hbm, remap_target),
                (counts_hbm, remap_counts),
                (coupling_hbm, coupling),
                (halo_rows_hbm, halo_rows),
                (halo_send_hbm.at[0], picks_smem),
                (halo_send_hbm.at[0], halo_send),
                (halo_ghost_hbm.at[0], halo_ghost),
            ]
        )
    ]
    for copy in small:
        copy.start()
    part, span = blocks // CHUNKS, cells // CHUNKS
    loads = {}

    def load(t):
        for chunk in range(CHUNKS):
            run = pl.ds(chunk * span, span)
            bunch = pl.ds(chunk * part, part)
            if t == 0:
                loads[chunk] = pltpu.make_async_copy(
                    inverse_hbm.at[bunch], inverse.at[bunch], load_sem.at[chunk]
                )
                loads[chunk].start()
            loads[t, chunk] = pltpu.make_async_copy(
                tracer_hbm.at[t, :, run],
                tracer.at[t, :, run],
                load_sem.at[(1 + t) * CHUNKS + chunk],
            )
            loads[t, chunk].start()

    load(0)
    weight_load = pltpu.make_async_copy(
        weights_hbm.at[0], weights, load_sem.at[(1 + tracers) * CHUNKS]
    )
    for copy in small[:2]:
        copy.wait()
    for a in range(atm_blocks.shape[0]):
        atm_blocks[a] = atm[:, a * block : (a + 1) * block]
    for d in range(spans):
        for c in range(slots):
            piece = atm_blocks[remap_send[d, 0, c]]
            if d == radius:
                arrived[d, c] = piece
            else:
                outgoing[d, c] = piece

    for t in range(1, tracers):
        load(t)
    weight_load.start()
    low = me < radius
    order = [h for h in range(hosts) if steps[h] > 0]
    order += [h for h in range(hosts)[::-1] if steps[h] < 0]

    def remote(source, target, sems, index, h):
        return pltpu.make_async_remote_copy(
            src_ref=source,
            dst_ref=target,
            send_sem=sems[0].at[index],
            recv_sem=sems[1].at[index],
            device_id=(peer(steps[h]),),
            device_id_type=MESH,
        )

    def flux_copy(h):
        d = steps[h] + radius
        return remote(outgoing.at[d], arrived.at[d], (flux_send_sem, flux_recv_sem), h, h)

    def row_copy(h, t):
        level = pl.ds(t * levels, levels)
        return remote(
            picked.at[h, level], received.at[h, level], (halo_send_sem, halo_recv_sem), (h, t), h
        )

    def side_copy(h, kind):
        source, target = (
            (tips, tips_in.at[h]),
            (halo_send.at[h], cells_in.at[h]),
            (surface_out.at[h], surface_in.at[h]),
        )[kind]
        return remote(source, target, (side_send_sem, side_recv_sem), (kind, h), h)

    far_first = sorted(range(hosts), key=lambda h: -abs(steps[h]))
    ahead = [h for h in range(hosts) if steps[h] > 0]

    @pl.when(jnp.logical_not(low))
    def _():
        pl.semaphore_wait(barrier, len(steps))
        for h in far_first:
            flux_copy(h).start()
        for h in ahead:

            @pl.when(me - steps[h] < radius)
            def _():
                pl.semaphore_signal(
                    ready.at[h],
                    inc=1,
                    device_id=(peer(-steps[h]),),
                    device_id_type=MESH,
                )

    lane = lax.broadcasted_iota(jnp.int32, (levels, block), 1)

    def mix_block(k, t):
        run = slice(k * block, (k + 1) * block)
        if t == 0:
            full = inverse[k]
            high, low_part = split(full)
            left = jnp.concatenate([high, low_part, high], axis=1)
            factor[k] = left
            first = jnp.broadcast_to(full[:, 0:1], (levels, block))
            if k % block == 0:
                column[k // block] = first
            else:
                column[k // block] = jnp.where(lane == k % block, first, column[k // block])
        else:
            left = factor[k]
        held = tracer[t, :, run]
        right_high, right_low = split(held)
        solved = product(left, jnp.concatenate([right_high, right_high, right_low], axis=0))
        value = jnp.where(wet[0:1, run] != 0, solved, held)
        mixed[t, :, run] = value
        base_rows[t, run, :] = jnp.transpose(value)
    small[2].wait()
    for chunk in range(CHUNKS):
        loads[chunk].wait()
        loads[0, chunk].wait()
        for k in range(chunk * part, (chunk + 1) * part):
            mix_block(k, 0)
    for copy in small[3:]:
        copy.wait()
    held_back = [(h, tracers - 1) for h in order if steps[h] < 0]
    flat = jnp.concatenate([jnp.transpose(column[i]) for i in range(column.shape[0])], axis=0)
    tips[...] = flat[:blocks].astype(jnp.bfloat16)
    sent = {h: [] for h in range(hosts)}
    unsent = {}
    for t in range(tracers):
        if t > 0:
            for chunk in range(CHUNKS):
                loads[t, chunk].wait()
            for k in range(blocks):
                mix_block(k, t)
        for h in order:
            for row in range(picks):
                cell = picks_smem[h, row // lanes, row % lanes]
                gathered[row] = base_rows[t, cell]
            picked[h, t * levels : (t + 1) * levels, :] = jnp.transpose(gathered[...]).astype(
                jnp.bfloat16
            )
            bundle = [row_copy(h, t)] if (h, t) not in held_back else []
            if t == 0:
                bundle += [side_copy(h, 0), side_copy(h, 1)]
            go = jnp.logical_not(low)
            if h in ahead and t == 0:
                near = jnp.logical_and(low, me + steps[h] >= radius)

                @pl.when(near)
                def _():
                    pl.semaphore_wait(ready.at[h], 1)
                    flux_copy(h).start()

                go = jnp.logical_or(go, near)

            @pl.when(go)
            def _():
                for copy in bundle:
                    copy.start()

            if h not in ahead or t > 0:
                sent[h] += bundle
            else:
                unsent[h] = bundle

    @pl.when(low)
    def _():
        pl.semaphore_wait(barrier, len(steps))
        for h in far_first:
            if h in ahead:

                @pl.when(me + steps[h] < radius)
                def _():
                    flux_copy(h).start()
                    for copy in unsent[h]:
                        copy.start()

            else:
                flux_copy(h).start()
        for h in order:
            for copy in sent[h]:
                copy.start()
    weight_load.wait()
    owner = lax.broadcasted_iota(jnp.int32, (blocks, fluxes, block), 0)
    blank = jnp.zeros((fluxes, block), jnp.int32)
    early_spans = [d for d in range(spans) if d >= radius]
    for group in (early_spans, [d for d in range(spans) if d < radius]):
        for d in group:
            if d != radius:
                flux_copy(steps.index(d - radius)).wait_recv()
        lefts = []
        for d in group:
            for c in range(slots):
                used = (blank + remap_counts[0, d]) > c
                piece = jnp.where(used, arrived[d, c].astype(jnp.float32), 0.0)
                placed = jnp.where(owner == remap_target[d, 0, c], piece[None], 0.0)
                lefts.append(placed.reshape(blocks * fluxes, block).astype(jnp.bfloat16))
        term = product(
            jnp.concatenate(lefts, axis=1),
            weights[group[0] : group[-1] + 1].reshape(len(group) * slots * block, block),
        )
        if group is early_spans:
            total[...] = term
        else:
            total[...] += term
    pad = surface.shape[0] - tracers
    for b in range(blocks):
        run = slice(b * block, (b + 1) * block)
        flux = total[b * fluxes : (b + 1) * fluxes, :] * wet[0:1, run].astype(jnp.float32)
        flux_out[:, run] = flux
        rows = []
        for t in range(tracers):
            value = coupling[t, 0] * flux[0:1, :]
            for f in range(1, fluxes):
                value = value + coupling[t, f] * flux[f : f + 1, :]
            rows.append(value)
        stacked = jnp.concatenate(rows + [jnp.zeros((pad, block), jnp.float32)], axis=0)
        surface[:, run] = stacked
        surface_rows[run, :] = jnp.transpose(stacked)
    for h in order:
        for row in range(picks):
            cell = picks_smem[h, row // lanes, row % lanes]
            surface_gathered[row] = surface_rows[cell]
        surface_out[h] = jnp.transpose(surface_gathered[...])[:tracers]
        side_copy(h, 2).start()
    for h, t in held_back:
        row_copy(h, t).start()
    ghosts = []
    line = jnp.zeros((1, lanes), jnp.int32)
    for h in range(hosts):
        for r in range(depth):
            used = (line + halo_rows[0, h]) > r
            ghosts.append(jnp.where(used, halo_ghost[h, r : r + 1, :], -1))
    places = jnp.transpose(jnp.concatenate(ghosts, axis=0))
    rows = min(TILE, cells)
    ones = jnp.ones((16, len(ghosts) * lanes), jnp.bfloat16)
    marks = [
        jnp.broadcast_to(places[:, i : i + 1], (lanes, rows)).astype(jnp.int16)
        for i in range(len(ghosts))
    ]
    ids = lax.broadcasted_iota(jnp.int32, (lanes, rows), 1).astype(jnp.int16)
    for index in range(cells // rows):
        run = slice(index * rows, (index + 1) * rows)
        pull = jnp.broadcast_to(0.25 * wet[0:1, run].astype(jnp.float32), (lanes, rows)).astype(
            jnp.bfloat16
        )
        here = ids + jnp.int16(index * rows)
        for i in range(len(ghosts)):
            scatter[i * lanes : (i + 1) * lanes, run] = jnp.where(
                here == marks[i], pull, jnp.bfloat16(0)
            )
        keep[:, run] = 1.0 - product(ones, scatter[:, run])[0:1]
    for k in range(blocks):
        run = slice(k * block, (k + 1) * block)
        first = jnp.broadcast_to(inverse[k, :, 0:1], (levels, block))
        for t in range(tracers):
            mixed[t, :, run] = keep[:, run] * (
                mixed[t, :, run] + first * surface[t : t + 1, run]
            )

    ids = lax.broadcasted_iota(jnp.int32, (blocks, picks), 0)
    shift = block.bit_length() - 1

    half = hosts // 2
    first_half = jnp.where(low, 0, half)

    def correct(start, target):
        for i in range(half):
            h = start + i
            for kind, (source, landing) in enumerate(
                ((tips, tips_in), (halo_send.at[0], cells_in), (surface_out.at[0], surface_in))
            ):
                pltpu.make_async_remote_copy(
                    src_ref=source,
                    dst_ref=landing.at[h],
                    send_sem=side_send_sem.at[kind, h],
                    recv_sem=side_recv_sem.at[kind, h],
                    device_id=(peer(1),),
                    device_id_type=MESH,
                ).wait_recv()
            for t in range(tracers):
                level = pl.ds(t * levels, levels)
                pltpu.make_async_remote_copy(
                    src_ref=picked.at[0, level],
                    dst_ref=received.at[h, level],
                    send_sem=halo_send_sem.at[h, t],
                    recv_sem=halo_recv_sem.at[h, t],
                    device_id=(peer(1),),
                    device_id_type=MESH,
                ).wait_recv()
        for i in range(half):
            h = start + i
            numbers = cells_in[h]
            where = jnp.concatenate([numbers[r : r + 1, :] for r in range(depth)], axis=1)
            hit = ids == lax.shift_right_logical(where, shift)
            tip = lax.dot_general(
                tips_in[h],
                jnp.where(hit, 1.0, 0.0).astype(jnp.bfloat16),
                (((0,), (0,)), ((), ())),
                preferred_element_type=jnp.float32,
            )
            tendency = surface_in[h]
            for t in range(tracers):
                level = slice(t * levels, (t + 1) * levels)
                value = received[h, level, :].astype(jnp.float32) + tip * tendency[t : t + 1, :]
                target[level, i * picks : (i + 1) * picks] = value.astype(jnp.bfloat16)

    correct(first_half, early_values)
    area = pl.ds(pl.multiple_of(first_half * picks, half * picks), half * picks)
    for index in range(cells // rows):
        run = slice(index * rows, (index + 1) * rows)
        summed = product(early_values[...], scatter[area, run])
        for t in range(tracers):
            mixed[t, :, run] += summed[t * levels : (t + 1) * levels]
    correct(half - first_half, values)
    for h in range(hosts):
        flux_copy(h).wait_send()
        for t in range(tracers):
            row_copy(h, t).wait_send()
        for kind in range(3):
            side_copy(h, kind).wait_send()


def halo_kernel(radius, values, scatter, kept, flux_in, flux_out, out, stage, sems):
    tracers, levels, cells = out.shape
    count = values.shape[1]
    start = jnp.where(lax.axis_index("patch") < radius, count, 0)
    area = pl.ds(pl.multiple_of(start, count), count)
    flux_copy = pltpu.make_async_copy(flux_in, flux_out, sems.at[0])
    flux_copy.start()
    tile = min(TILE, cells)
    copies = [flux_copy]
    for index in range(cells // tile):
        run = slice(index * tile, (index + 1) * tile)
        summed = product(values[...], scatter[area, run])
        for t in range(tracers):
            stage[t, :, run] = kept[t, :, run] + summed[t * levels : (t + 1) * levels]
        place = pl.ds(index * tile, tile)
        copy = pltpu.make_async_copy(
            stage.at[:, :, place], out.at[:, :, place], sems.at[1 + index]
        )
        copy.start()
        copies.append(copy)
    for copy in copies:
        copy.wait()


def body(
    atm_flux,
    remap_send,
    remap_target,
    remap_counts,
    remap_weights,
    coupling,
    tracer,
    wet,
    mix_inverse,
    halo_send,
    halo_ghost,
    halo_rows,
):
    spans, slots = remap_send.shape[1:]
    block = remap_weights.shape[-1]
    fluxes = atm_flux.shape[0]
    tracers, levels, cells = tracer.shape
    blocks = cells // block
    hosts, depth, lanes = halo_send.shape[1:]
    picks = depth * lanes
    features = tracers * levels
    lead = -(-tracers // 8) * 8
    vmem = pl.BlockSpec(memory_space=pltpu.VMEM)
    hbm = pl.BlockSpec(memory_space=pltpu.HBM)
    dma = pltpu.SemaphoreType.DMA
    flux, kept, values, scatter = pl.pallas_call(
        couple_kernel,
        out_shape=(
            pltpu.VMEM((fluxes, cells), jnp.float32),
            pltpu.VMEM((tracers, levels, cells), jnp.float32),
            pltpu.VMEM((features, hosts // 2 * picks), jnp.bfloat16),
            pltpu.VMEM((hosts * picks, cells), jnp.bfloat16),
        ),
        in_specs=[hbm] * 12,
        out_specs=(vmem, vmem, vmem, vmem),
        scratch_shapes=[
            pltpu.SMEM((spans, 1, slots), jnp.int32),
            pltpu.SMEM((spans, 1, slots), jnp.int32),
            pltpu.SMEM((1, spans), jnp.int32),
            pltpu.SMEM((tracers, fluxes), jnp.float32),
            pltpu.SMEM((1, hosts), jnp.int32),
            pltpu.SMEM((hosts, depth, lanes), jnp.int32),
            pltpu.VMEM(atm_flux.shape, jnp.bfloat16),
            pltpu.VMEM((atm_flux.shape[1] // block, fluxes, block), jnp.bfloat16),
            pltpu.VMEM((1, cells), jnp.int32),
            pltpu.VMEM((hosts, depth, lanes), jnp.int32),
            pltpu.VMEM((hosts, depth, lanes), jnp.int32),
            pltpu.VMEM((spans, slots, block, block), jnp.bfloat16),
            pltpu.VMEM((tracers, levels, cells), jnp.float32),
            pltpu.VMEM((blocks, levels, levels), jnp.float32),
            pltpu.VMEM((tracers, cells, levels), jnp.float32),
            pltpu.VMEM((picks, levels), jnp.float32),
            pltpu.VMEM((features, hosts // 2 * picks), jnp.bfloat16),
            pltpu.VMEM((blocks, levels, 3 * levels), jnp.bfloat16),
            pltpu.VMEM((1, cells), jnp.float32),
            pltpu.VMEM((lead, cells), jnp.float32),
            pltpu.VMEM((cells, lead), jnp.float32),
            pltpu.VMEM((picks, lead), jnp.float32),
            pltpu.VMEM((hosts, tracers, picks), jnp.float32),
            pltpu.VMEM((hosts, tracers, picks), jnp.float32),
            pltpu.VMEM((blocks * fluxes, block), jnp.float32),
            pltpu.VMEM((spans, slots, fluxes, block), jnp.bfloat16),
            pltpu.VMEM((spans, slots, fluxes, block), jnp.bfloat16),
            pltpu.VMEM((hosts, features, picks), jnp.bfloat16),
            pltpu.VMEM((hosts, features, picks), jnp.bfloat16),
            pltpu.VMEM((-(-blocks // block), levels, block), jnp.float32),
            pltpu.VMEM((blocks, levels), jnp.bfloat16),
            pltpu.VMEM((hosts, blocks, levels), jnp.bfloat16),
            pltpu.VMEM((hosts, depth, lanes), jnp.int32),
            dma(((1 + tracers) * CHUNKS + 1,)),
            dma((10,)),
            dma((hosts,)),
            dma((hosts,)),
            dma((hosts, tracers)),
            dma((hosts, tracers)),
            dma((3, hosts)),
            dma((3, hosts)),
            pltpu.SemaphoreType.REGULAR((hosts,)),
        ],
        compiler_params=pltpu.CompilerParams(
            collective_id=0, has_side_effects=True, vmem_limit_bytes=48 * 1024 * 1024
        ),
        name="couple",
    )(
        remap_send.transpose(1, 0, 2),
        remap_target.transpose(1, 0, 2),
        remap_counts,
        coupling,
        halo_rows,
        atm_flux,
        wet.reshape(1, cells),
        halo_send,
        halo_ghost,
        remap_weights,
        tracer,
        mix_inverse,
    )
    tile = min(TILE, cells)
    return pl.pallas_call(
        functools.partial(halo_kernel, spans // 2),
        out_shape=(
            jax.ShapeDtypeStruct((fluxes, cells), jnp.float32),
            jax.ShapeDtypeStruct((tracers, levels, cells), jnp.float32),
        ),
        in_specs=[vmem] * 4,
        out_specs=(hbm, hbm),
        scratch_shapes=[
            pltpu.VMEM((tracers, levels, cells), jnp.float32),
            dma((1 + cells // tile,)),
        ],
        compiler_params=pltpu.CompilerParams(vmem_limit_bytes=24 * 1024 * 1024),
        name="halo",
    )(values, scatter, kept, flux)


def solution(mesh):
    return jax.shard_map(
        body,
        mesh=mesh,
        in_specs=(
            P(None, "patch"),
            P("patch", None, None),
            P("patch", None, None),
            P("patch", None),
            P("patch", None, None, None, None),
            P(),
            P(None, None, "patch"),
            P("patch"),
            P("patch", None, None),
            P("patch", None, None, None),
            P("patch", None, None, None),
            P("patch", None),
        ),
        out_specs=(P(None, "patch"), P(None, None, "patch")),
        check_vma=False,
    )
```
